32 devices in a mesh: expert: 4 (over y, core), shard: 8 (over z, x).
Axes of the slice: x: 2, y: 2, z: 4, core: 2. Of those that a mesh axis runs over, the one named last changes fastest.
Arguments:
- w_gate: float32 [128, 2048, 768], P('expert', 'shard'), may hold values from -0.1875 to 0.1875
- w_up: float32 [128, 2048, 768], P('expert', 'shard'), may hold values from -0.1875 to 0.1875
- router_weight: float32 [2048, 128], P('shard', 'expert'), may hold values from -0.125 to 0.125
- router_gain: float32 [2048], P('shard'), may hold values from 0.25 to 1.75
Outputs:
- serve_gate: bfloat16 [128, 2048, 768], P('expert', None, 'shard')
- serve_up: bfloat16 [128, 2048, 768], P('expert', None, 'shard')
- scale_gate: float32 [128, 768], P('expert', 'shard')
- scale_up: float32 [128, 768], P('expert', 'shard')
- serve_router: bfloat16 [2048, 128], replicated
The draws below stay inside these ranges and needn't reach their ends.
All inputs are finite; a program needn't handle non-finite values. Where the reference program divides by a largest or mean magnitude, that divisor is 1e-20 or more.
Results may differ from the reference program's by a relative error of at most 0.001.
Values may be sent and summed in bfloat16 or wider, within the bound.
A program may use at most 192 MiB of HBM per device.

```python
import jax
import jax.numpy as jnp

EXPERTS = 128
D_MODEL = 2048
D_EXPERT = 768


def with_spikes(result, stream_key, source, target, blocks, factor):
    def block_of(dim):
        return (jnp.arange(result.shape[dim]) // (result.shape[dim] // blocks)).reshape((-1,) + (1,) * (result.ndim - 1 - dim))

    near = jax.random.permutation(stream_key, blocks)[block_of(target)]
    other_side = (block_of(target) + blocks // 2) % blocks
    return jnp.where((block_of(source) == near) | (block_of(source) == other_side), factor * result, result)


def block_levels(rng, shape, cuts, low, largest):
    loudness, own = 1.0, jax.random.fold_in(rng, 6)
    for dim, blocks in cuts:
        steps = jnp.exp(jax.random.uniform(jax.random.fold_in(own, dim), (blocks,), jnp.float32, low / len(cuts), largest / len(cuts)))
        loudness = loudness * jnp.repeat(steps, shape[dim] // blocks).reshape([-1 if axis == dim else 1 for axis in range(len(shape))])
    return loudness


def normal_values(key, shape, deviation, reach, split=(), kind=jnp.bfloat16):
    loudness = block_levels(key, shape, split, -0.22, 0.18) if split else 1.0
    result = jax.random.normal(key, shape, jnp.float32) * deviation * loudness
    return jnp.minimum(jnp.maximum(result, -reach), reach).astype(kind)


def bell_draw_with(key, dims, width, most, cuts, heavy, dtype=jnp.bfloat16):
    result = width * jax.random.normal(key, dims, jnp.float32)
    if cuts:
        result = result * block_levels(key, dims, cuts, -0.22, 0.18)
    return jnp.clip(with_spikes(result, jax.random.fold_in(key, 3), *heavy), -most, most).astype(dtype)


def setup_inputs(seed: int = 0) -> dict:
    arg_keys = jax.random.split(jax.random.key(seed), 5)
    w_gate = bell_draw_with(arg_keys[0], (EXPERTS, D_MODEL, D_EXPERT), D_MODEL ** -0.5, 0.1875, ((0, 4), (1, 8)), (1, 2, 8, 2.0), jnp.float32)
    w_up = bell_draw_with(arg_keys[1], (EXPERTS, D_MODEL, D_EXPERT), D_MODEL ** -0.5, 0.1875, ((0, 4), (1, 8)), (1, 2, 8, 2.0), jnp.float32)
    router_weight = normal_values(arg_keys[2], (D_MODEL, EXPERTS), D_MODEL ** -0.5, 0.125, ((0, 8), (1, 4)), jnp.float32)
    router_gain = jnp.clip(1.0 + 0.15 * jax.random.normal(arg_keys[3], (D_MODEL,), jnp.float32), 0.25, 1.75)
    return dict(w_gate=w_gate, w_up=w_up, router_weight=router_weight, router_gain=router_gain)


def reference(w_gate, w_up, router_weight, router_gain):
    scale_gate = jnp.max(jnp.abs(w_gate), axis=1)
    serve_gate = (w_gate / jnp.expand_dims(scale_gate, 1)).astype(jnp.bfloat16)
    scale_up = jnp.max(jnp.abs(w_up), axis=1)
    serve_up = (w_up / jnp.expand_dims(scale_up, 1)).astype(jnp.bfloat16)
    serve_router = (router_weight * router_gain[:, None]).astype(jnp.bfloat16)
    return serve_gate, serve_up, scale_gate, scale_up, serve_router
```

```python
import functools
import math

import jax
import jax.numpy as jnp
from jax import lax
from jax.experimental import pallas as pl
from jax.experimental.pallas import tpu as pltpu
from jax.sharding import PartitionSpec as P

MESH = pl.DeviceIdType.MESH
SLOTS = 4
LANES = 128


def kernel(
    n, ne, chunk,
    gate, up, router, gain,
    out_gate, out_up, out_scale, out_router,
    ring, send, lmax, rs, gm, rbuf,
    load_sem, own_sem, send_sem, recv_sem,
    rs_send, rs_recv, ag_send, ag_recv,
    r1_send, r1_recv, r2_send, r2_recv,
):
    me = lax.axis_index("shard")
    my_e = lax.axis_index("expert")
    experts, rows, cols = gate.shape
    part = cols // n
    share = experts // n
    chunks = experts // chunk
    outs = (out_gate, out_up)

    offsets = sorted(range(1, n), key=lambda r: (abs(r - n // 2), r))

    def ahead(r):
        return lax.rem(me + r, n)

    def behind(r):
        return lax.rem(me + (n - r), n)

    def load(array, index, slot):
        return pltpu.make_async_copy(
            array.at[pl.ds(index * chunk, chunk)], ring.at[slot], load_sem.at[slot]
        )

    def start_load(k):
        slot, index, which = k % SLOTS, k % chunks, (k // chunks) % 2

        @pl.when((k < 4 * chunks) & (which == 0))
        def _():
            load(gate, index, slot).start()

        @pl.when((k < 4 * chunks) & (which == 1))
        def _():
            load(up, index, slot).start()

    for k in range(SLOTS):
        load((gate, up)[(k // chunks) % 2], k % chunks, k).start()

    barrier = pltpu.get_barrier_semaphore()
    for r in range(1, n):
        pl.semaphore_signal(barrier, inc=1, device_id={"shard": ahead(r)}, device_id_type=MESH)
    for r in range(1, ne):
        pl.semaphore_signal(
            barrier, inc=1, device_id={"expert": lax.rem(my_e + r, ne)}, device_id_type=MESH
        )

    rbuf[my_e, me] = (router[...] * gain[...]).astype(jnp.bfloat16)

    pl.semaphore_wait(barrier, n + ne - 2)

    def router_row(r, slot):
        return pltpu.make_async_remote_copy(
            src_ref=rbuf.at[my_e, me], dst_ref=rbuf.at[my_e, slot],
            send_sem=r1_send.at[r], recv_sem=r1_recv.at[r],
            device_id={"shard": ahead(r)}, device_id_type=MESH,
        )

    def router_col(r, slot):
        return pltpu.make_async_remote_copy(
            src_ref=rbuf.at[my_e], dst_ref=rbuf.at[slot],
            send_sem=r2_send.at[r], recv_sem=r2_recv.at[r],
            device_id={"expert": lax.rem(my_e + r, ne)}, device_id_type=MESH,
        )

    def spread(a, r, slot):
        return pltpu.make_async_remote_copy(
            src_ref=lmax.at[a, pl.ds(ahead(r) * share, share)], dst_ref=rs.at[a, slot],
            send_sem=rs_send.at[a, r], recv_sem=rs_recv.at[a, r],
            device_id={"shard": ahead(r)}, device_id_type=MESH,
        )

    def collect(a, r, slot):
        return pltpu.make_async_remote_copy(
            src_ref=gm.at[a, pl.ds(me * share, share)],
            dst_ref=gm.at[a, pl.ds(slot * share, share)],
            send_sem=ag_send.at[a, r], recv_sem=ag_recv.at[a, r],
            device_id={"shard": ahead(r)}, device_id_type=MESH,
        )

    def column(slot):
        return pl.ds(pl.multiple_of(slot * rows, LANES), rows)

    def peer_rows(slot):
        return pl.ds(pl.multiple_of(slot * part, 16), part)

    def piece(a, r, slot, first, count):
        return pltpu.make_async_remote_copy(
            src_ref=send.at[a, pl.ds(first, count), peer_rows(ahead(r))],
            dst_ref=outs[a].at[pl.ds(first, count), :, column(slot)],
            send_sem=send_sem.at[a, r], recv_sem=recv_sem.at[a, r],
            device_id={"shard": ahead(r)}, device_id_type=MESH,
        )

    def own(a, first, count):
        return pltpu.make_async_copy(
            send.at[a, pl.ds(first, count), peer_rows(me)],
            outs[a].at[pl.ds(first, count), :, column(me)],
            own_sem.at[a],
        )

    def maxima(a):
        @pl.loop(0, chunks)
        def _(c):
            k = a * chunks + c
            slot = k % SLOTS
            load(gate, 0, slot).wait()

            @pl.loop(0, chunk)
            def _(i):
                lmax[a, c * chunk + i] = jnp.max(jnp.abs(ring[slot, i]), axis=0, keepdims=True)

            start_load(k + SLOTS)

    def reduce(a):
        largest = lmax[a, pl.ds(me * share, share)]
        for r in offsets:
            spread(a, r, behind(r)).wait_recv()
            largest = jnp.maximum(largest, rs[a, behind(r)])
        gm[a, pl.ds(me * share, share)] = largest

    def ship(a, first):
        for r in offsets:
            piece(a, r, me, first, chunk).start()
        own(a, first, chunk).start()

    def quotients(a):
        @pl.loop(0, chunks)
        def _(c):
            k = (2 + a) * chunks + c
            slot = k % SLOTS
            load(gate, 0, slot).wait()

            @pl.loop(0, chunk)
            def _(i):
                e = c * chunk + i
                inverse = 1.0 / gm[a, e]
                for j in range(0, cols, LANES):
                    block = ring[slot, i, :, j:j + LANES] * inverse[:, j:j + LANES]
                    send[a, e, j:j + LANES, :] = block.T.astype(jnp.bfloat16)

            start_load(k + SLOTS)

            @pl.when(c > 0)
            def _():
                ship(a, (c - 1) * chunk)

        ship(a, (chunks - 1) * chunk)

    for r in offsets:
        router_row(r, me).start()
    maxima(0)
    for r in offsets:
        spread(0, r, me).start()
    maxima(1)
    for r in offsets:
        spread(1, r, me).start()
    reduce(0)
    for r in offsets:
        collect(0, r, me).start()
    reduce(1)
    for r in offsets:
        collect(1, r, me).start()
    for r in offsets:
        collect(0, r, behind(r)).wait_recv()
    quotients(0)
    for r in offsets:
        collect(1, r, behind(r)).wait_recv()
    quotients(1)

    for r in offsets:
        router_row(r, behind(r)).wait_recv()
    for r in range(1, ne):
        router_col(r, my_e).start()
    out_scale[...] = gm[...]
    for r in range(1, ne):
        router_col(r, lax.rem(my_e + (ne - r), ne)).wait_recv()
    for s in range(n):
        block = rbuf[:, s].astype(jnp.float32).reshape(ne * rbuf.shape[2], rows)
        out_router[s * rows:(s + 1) * rows, :] = block.T.astype(jnp.bfloat16)

    for r in offsets:
        router_row(r, me).wait_send()
        for a in range(2):
            spread(a, r, me).wait_send()
            collect(a, r, me).wait_send()
    for r in range(1, ne):
        router_col(r, my_e).wait_send()
    for a in range(2):
        own(a, 0, experts).wait()
        for r in offsets:
            piece(a, r, me, 0, experts).wait_send()
            piece(a, r, behind(r), 0, experts).wait_recv()


def plain_body(w_gate, w_up, router_weight, router_gain):
    scale_gate, scale_up = lax.pmax(
        (jnp.max(jnp.abs(w_gate), axis=1), jnp.max(jnp.abs(w_up), axis=1)), "shard"
    )
    narrow_gate, narrow_up = (
        (w_gate / jnp.expand_dims(scale_gate, 1)).astype(jnp.bfloat16),
        (w_up / jnp.expand_dims(scale_up, 1)).astype(jnp.bfloat16),
    )
    serve_gate, serve_up = (
        lax.all_to_all(narrow_gate, "shard", split_axis=2, concat_axis=1, tiled=True),
        lax.all_to_all(narrow_up, "shard", split_axis=2, concat_axis=1, tiled=True),
    )
    scale_gate = lax.dynamic_slice_in_dim(
        scale_gate, lax.axis_index("shard") * serve_gate.shape[2], serve_gate.shape[2], axis=1
    )
    scale_up = lax.dynamic_slice_in_dim(
        scale_up, lax.axis_index("shard") * serve_up.shape[2], serve_up.shape[2], axis=1
    )
    part_router = (router_weight * router_gain[:, None]).astype(jnp.bfloat16)
    row_router = lax.all_gather(part_router, "shard", axis=0, tiled=True)
    serve_router = lax.all_gather(row_router, "expert", axis=1, tiled=True)
    return (serve_gate, serve_up, scale_gate, scale_up, serve_router)


def body(n, ne, w_gate, w_up, router_weight, router_gain):
    experts, rows, cols = w_gate.shape
    if rows % LANES or cols % LANES or (cols // n) % 16 or experts % n:
        return plain_body(w_gate, w_up, router_weight, router_gain)
    part, share = cols // n, experts // n
    chunk = math.gcd(experts, 4)
    serve = jax.ShapeDtypeStruct((experts, part, n * rows), jnp.bfloat16)
    dma = pltpu.SemaphoreType.DMA
    anywhere = pl.BlockSpec(memory_space=pl.ANY)
    local = pl.BlockSpec(memory_space=pltpu.VMEM)
    gate, up, scale, router = pl.pallas_call(
        functools.partial(kernel, n, ne, chunk),
        out_shape=(
            serve,
            serve,
            jax.ShapeDtypeStruct((2, experts, 1, cols), jnp.float32),
            jax.ShapeDtypeStruct((n * rows, ne * router_weight.shape[1]), jnp.bfloat16),
        ),
        in_specs=[anywhere, anywhere, local, local],
        out_specs=(anywhere, anywhere, local, local),
        scratch_shapes=[
            pltpu.VMEM((SLOTS, chunk, rows, cols), jnp.float32),
            pltpu.VMEM((2, experts, cols, rows), jnp.bfloat16),
            pltpu.VMEM((2, experts, 1, cols), jnp.float32),
            pltpu.VMEM((2, n, share, 1, cols), jnp.float32),
            pltpu.VMEM((2, experts, 1, cols), jnp.float32),
            pltpu.VMEM((ne, n, router_weight.shape[1], rows), jnp.bfloat16),
            dma((SLOTS,)),
            dma((2,)),
            dma((2, n)),
            dma((2, n)),
            dma((2, n)),
            dma((2, n)),
            dma((2, n)),
            dma((2, n)),
            dma((n,)),
            dma((n,)),
            dma((ne,)),
            dma((ne,)),
        ],
        compiler_params=pltpu.CompilerParams(
            collective_id=0, has_side_effects=True, vmem_limit_bytes=60 * 2**20
        ),
        cost_estimate=pl.CostEstimate(
            flops=4 * experts * rows * cols, bytes_accessed=20 * experts * rows * cols, transcendentals=0
        ),
    )(w_gate, w_up, router_weight.T, router_gain[None, :])
    first = lax.axis_index("shard") * part
    scale = lax.dynamic_slice_in_dim(scale[:, :, 0, :], first, part, axis=2)
    return (jnp.swapaxes(gate, 1, 2), jnp.swapaxes(up, 1, 2), scale[0], scale[1], router)


def solution(mesh):
    return jax.shard_map(
        functools.partial(body, mesh.shape["shard"], mesh.shape["expert"]),
        mesh=mesh,
        in_specs=(
            P("expert", "shard", None),
            P("expert", "shard", None),
            P("shard", "expert"),
            P("shard"),
        ),
        out_specs=(
            P("expert", None, "shard"),
            P("expert", None, "shard"),
            P("expert", "shard"),
            P("expert", "shard"),
            P(),
        ),
        check_vma=False,
    )
```
